32 devices in a mesh: tm: 16 (over z, x, core), space: 2 (over y).
Axes of the slice: x: 2, y: 2, z: 4, core: 2. Of those that a mesh axis runs over, the one named last changes fastest.
Arguments:
- forcing: float32 [16, 8, 128, 128], P('tm', 'space'), may hold values from -6 to 6
- initial: float32 [8, 128, 128], P('space'), may hold values from -6 to 6
- coupling: float32 [8, 128, 128], P('space'), may hold values from 0.3 to 3
- velocity: float32 [3, 8, 128, 128], P(None, 'space'), may hold values from -0.9 to 0.9
Outputs:
- iterate: float32 [16, 8, 128, 128], P('tm', 'space')
The draws below stay inside these ranges and needn't reach their ends.
All inputs are finite; a program needn't handle non-finite values.
Results may differ from the reference program's by a relative error of at most 0.0003.
Values sent between devices are 32-bit elements; how exact they have to be, the bound alone decides.
No kernel may reach another device: no remote copies, remote signals or barrier semaphores. Data moves between devices by JAX's collectives and lax.ppermute only.
A program may use at most 64 MiB of HBM per device.

```python
import math
import jax
import jax.numpy as jnp
from jax import lax

NY = 128
NX = 128
ITERS = 2
SWEEPS = 8
NT = 16
NZ = 8


def level_of(stream_key, shape, cuts, low, top_value):
    level = 1.0
    for axis_at, parts in cuts:
        draws = jax.random.uniform(jax.random.fold_in(jax.random.fold_in(stream_key, 6), axis_at), (parts,), jnp.float32, low / len(cuts), top_value / len(cuts))
        level = level * jnp.repeat(jnp.exp(draws), shape[axis_at] // parts).reshape((-1,) + (1,) * (len(shape) - 1 - axis_at))
    return level


def gaussian(key, dims, width, reach, shards=(), kind=jnp.bfloat16):
    array = width * jax.random.normal(key, dims, jnp.float32)
    if shards:
        array = array * level_of(key, dims, shards, -0.22, 0.18)
    return jnp.clip(array, -reach, reach).astype(kind)


def setup_inputs(seed: int = 0) -> dict:
    arg_keys = jax.random.split(jax.random.key(seed), 5)
    forcing = gaussian(arg_keys[0], (NT, NZ, NY, NX), 1.0, 6.0, ((0, 16), (1, 2)), jnp.float32)
    initial = gaussian(arg_keys[1], (NZ, NY, NX), 1.0, 6.0, ((0, 2),), jnp.float32)
    coupling = jnp.clip(jnp.exp(math.log(3.0) - 2.3025851 * jax.random.uniform(arg_keys[2], (NZ, NY, NX), jnp.float32) ** level_of(arg_keys[2], (NZ, NY, NX), ((0, 2),), -0.2, 0.2)), 0.3, 3.0)
    velocity = jnp.clip(jax.random.uniform(arg_keys[3], (3, NZ, NY, NX), jnp.float32, -0.9, 0.9) * level_of(arg_keys[3], (3, NZ, NY, NX), ((1, 2),), -0.4, 0.0), -0.9, 0.9)
    return dict(forcing=forcing, initial=initial, coupling=coupling, velocity=velocity)


wrap_alpha = 0.1


def padded(field):
    widths = [(0, 0)] * (field.ndim - 3) + [(1, 1)] * 3
    return jnp.pad(field, widths)


def coupled(extended, coupling, advect):
    total = (coupling - advect[0]) * extended[..., 2:, 1:-1, 1:-1] + (coupling + advect[0]) * extended[..., :-2, 1:-1, 1:-1]
    total = total + (coupling - advect[1]) * extended[..., 1:-1, 2:, 1:-1] + (coupling + advect[1]) * extended[..., 1:-1, :-2, 1:-1]
    total = total + (coupling - advect[2]) * extended[..., 1:-1, 1:-1, 2:] + (coupling + advect[2]) * extended[..., 1:-1, 1:-1, :-2]
    return total


def tables(total_steps):
    indices = jnp.arange(total_steps, dtype=jnp.int32)
    products = (indices[:, None] * indices[None, :]) % total_steps
    angles = products.astype(jnp.float32) * (2.0 * math.pi / total_steps)
    return jnp.cos(angles), jnp.sin(angles)


def matmul(table, columns):
    return jnp.dot(table, columns, preferred_element_type=jnp.float32, precision=lax.Precision.HIGHEST)


def reference(forcing, initial, coupling, velocity):
    total_steps = forcing.shape[0]
    shape = forcing.shape
    advect = coupling[None] * velocity
    cosine, sine_table = tables(total_steps)
    steps_float = jnp.arange(total_steps, dtype=jnp.float32)
    time_weight = jnp.exp(math.log(wrap_alpha) * steps_float / total_steps)[:, None, None, None]
    radius = math.exp(math.log(wrap_alpha) / total_steps)
    angles = steps_float * (2.0 * math.pi / total_steps)
    shift_re = radius * jnp.cos(angles)
    shift_im = radius * jnp.sin(angles)
    iterate = jnp.broadcast_to(initial, shape).astype(jnp.float32)

    def solve(pieces):
        source_re, source_im, freq_re, freq_im = pieces
        diag_re = 1.0 + 6.0 * coupling - freq_re
        diag_im = freq_im
        modulus = diag_re * diag_re + diag_im * diag_im
        value_re = (source_re * diag_re + source_im * diag_im) / modulus
        value_im = (source_im * diag_re - source_re * diag_im) / modulus
        for sweep in range(SWEEPS):
            sum_re = source_re + coupled(padded(value_re), coupling, advect)
            sum_im = source_im + coupled(padded(value_im), coupling, advect)
            value_re = (sum_re * diag_re + sum_im * diag_im) / modulus
            value_im = (sum_im * diag_re - sum_re * diag_im) / modulus
        return value_re, value_im

    for repeat in range(ITERS):
        previous = jnp.concatenate([initial[None], iterate[:-1]], axis=0)
        residual = forcing - ((1.0 + 6.0 * coupling) * iterate - coupled(padded(iterate), coupling, advect)) + previous
        columns = (residual * time_weight).reshape(total_steps, -1)
        spec_re = matmul(cosine, columns).reshape(shape)
        spec_im = (-matmul(sine_table, columns)).reshape(shape)
        value_re, value_im = lax.map(solve, (spec_re, spec_im, shift_re, shift_im))
        inverse_part = (matmul(cosine, value_re.reshape(total_steps, -1)) - matmul(sine_table, value_im.reshape(total_steps, -1))) / total_steps
        iterate = iterate + inverse_part.reshape(shape) / time_weight
    return iterate
```

```python
import functools
import math

import jax
import jax.numpy as jnp
from jax import lax
from jax.experimental import pallas as pl
from jax.experimental.pallas import tpu as pltpu
from jax.sharding import PartitionSpec as P

ITERS = 2
SWEEPS = 8

wrap_alpha = 0.1

APPS = SWEEPS + 1
HALO = ITERS * APPS - 1
LANES = 128
SUB = 8


def position(site):
    a, b = site // 2, site % 2
    return 2 * a + (b ^ (a % 2))


def vmem_call(kernel, out_shapes, n_in, scratch=(), n_smem=0, flops=0, limit=None, name=None):
    specs = [pl.BlockSpec(memory_space=pltpu.SMEM)] * n_smem
    specs += [pl.BlockSpec(memory_space=pltpu.VMEM)] * n_in
    multi = isinstance(out_shapes, (tuple, list))
    outs = pl.BlockSpec(memory_space=pltpu.VMEM)
    return pl.pallas_call(
        kernel,
        out_shape=out_shapes,
        in_specs=specs,
        out_specs=[outs] * len(out_shapes) if multi else outs,
        scratch_shapes=list(scratch),
        compiler_params=pltpu.CompilerParams(vmem_limit_bytes=limit),
        cost_estimate=pl.CostEstimate(flops=flops, bytes_accessed=1 << 20, transcendentals=0),
        name=name,
    )


def pack_kernel(sites, rows, f_ref, o_ref):
    planes, total = f_ref.shape[0], f_ref.shape[1]
    block = (rows + 2) * planes
    for site in range(sites):
        first = position(site) * rows
        base = site * block
        for z in range(planes):
            for part in range(rows // SUB):
                tile = f_ref[z, pl.ds(first + part * SUB, SUB), :]
                o_ref[pl.ds(base + (1 + part * SUB) * planes + z, SUB, stride=planes), :] = tile
            for idx, row in ((0, first - 1), (rows + 1, first + rows)):
                if 0 <= row < total:
                    edge = f_ref[z, pl.ds(row, 1), :]
                else:
                    edge = jnp.zeros((1, LANES), jnp.float32)
                o_ref[pl.ds(base + idx * planes + z, 1), :] = edge


def unpack_kernel(sites, rows, ints, r_ref, i_ref, o_ref):
    core = ints[0]
    planes = i_ref.shape[0]
    half = rows // 2
    for site in range(sites):
        first = position(site) * rows
        for part in range(2):
            who = core if part == 0 else 1 - core
            base = (site * 2 + part) * half * planes
            for z in range(planes):
                for piece in range(half // SUB):
                    row = pl.multiple_of(first + who * half + piece * SUB, SUB)
                    tile = r_ref[pl.ds(base + piece * SUB * planes + z, SUB, stride=planes), :]
                    o_ref[0, z, pl.ds(row, SUB), :] = i_ref[z, pl.ds(row, SUB), :] + tile


def shifts(mid, low, high, coefs):
    depth = mid.shape[0]
    zp, zm, yp, ym, xp, xm = coefs
    out = zp * pltpu.roll(mid, depth - 1, 0) + zm * pltpu.roll(mid, 1, 0)
    out = out + (yp * high + ym * low)
    return out + (xp * pltpu.roll(mid, LANES - 1, 1) + xm * pltpu.roll(mid, 1, 1))


def prepare_coefs(coef_ref, row, c_ref, p_ref, dest, wrap, steps):
    coupling = coef_ref[row, 0]
    depth = coupling.shape[0]
    z = lax.broadcasted_iota(jnp.int32, coupling.shape, 0)
    x = lax.broadcasted_iota(jnp.int32, coupling.shape, 1)
    for k in range(3):
        advect = coupling * coef_ref[row, 1 + k]
        plus, minus = coupling - advect, coupling + advect
        if k == 0:
            plus = jnp.where(z == depth - 1, 0.0, plus)
            minus = jnp.where(z == 0, 0.0, minus)
        if k == 2:
            plus = jnp.where(x == LANES - 1, 0.0, plus)
            minus = jnp.where(x == 0, 0.0, minus)
        c_ref[dest, 2 * k] = plus
        c_ref[dest, 2 * k + 1] = minus
    inv = 1.0 / (1.0 + 6.0 * coupling)
    c_ref[dest, 6] = inv
    powers = [inv]
    for _ in range(steps - 1):
        powers.append(powers[-1] * inv)
    scale = wrap / (1.0 - wrap * powers[-1])
    for n in range(steps):
        p_ref[dest, n] = scale * powers[n]


def apply_rows(lo, count, steps, src, dst, s_ref, c_ref, p_ref, s_off, c_off, first):
    def row_body(i, carry):
        r = lo + i
        coefs = [c_ref[r - c_off, k] for k in range(6)]
        inv = c_ref[r - c_off, 6]
        run = None
        ys = []
        for n in range(steps):
            b = s_ref[r - s_off, n]
            if not first:
                b = b + shifts(src[r, n], src[r - 1, n], src[r + 1, n], coefs)
            run = b * inv if run is None else (b + run) * inv
            ys.append(run)
        for n in range(steps):
            dst[r, n] = ys[n] + ys[-1] * p_ref[r - c_off, n]
        return carry

    lax.fori_loop(0, count, row_body, 0)


def first_kernel(rows, steps, ints, floats, *refs):
    pieces, (coef_ref,) = refs[:12], refs[12:13]
    x_out, s_out, last_out = refs[13:16]
    s_ref, c_ref, p_ref, x0, x1, init_ref = refs[16:]
    core, side = ints[0], ints[1]
    wrap = floats[0]
    half = rows // 2
    own = half * core
    window = half + 2 * HALO
    margin = (coef_ref.shape[0] - rows) // 2
    sub = lax.broadcasted_iota(jnp.int32, (SUB, LANES), 0)

    def coef_body(i, carry):
        prepare_coefs(coef_ref, own + margin - HALO + i, c_ref, p_ref, i, wrap, steps)
        return carry

    lax.fori_loop(0, window, coef_body, 0)

    def source_body(i, carry):
        row = own + margin - HALO + i
        coefs = [c_ref[i, k] for k in range(6)]
        base = shifts(coef_ref[row, 4], coef_ref[row - 1, 4], coef_ref[row + 1, 4], coefs)
        base = base - 6.0 * coef_ref[row, 0] * coef_ref[row, 4]
        init_ref[i] = base * (1.0 + wrap)
        return carry

    lax.fori_loop(0, window, source_body, 0)

    for band, offset in ((0, 0), (1, -rows), (2, rows)):
        for who in range(2):
            keep, got = pieces[4 * band + 2 * who], pieces[4 * band + 2 * who + 1]
            parity = core if who == 0 else 1 - core
            for pair in range((rows + 2) // 2):
                for h in range(2):
                    row = offset + 2 * pair + h - 1
                    if band == 0 and not 0 <= row < rows:
                        continue
                    if band == 1 and row >= 0:
                        continue
                    if band == 2 and row < rows:
                        continue
                    at = row + HALO - own
                    ok = jnp.logical_and(at >= 0, at < window)

                    @pl.when(ok)
                    def _():
                        for i in range(steps // 2):
                            a, b = keep[i, pair], got[i, pair]
                            low = jnp.where(side == 0, a, b)
                            high = jnp.where(side == 0, b, a)
                            if h == 0:
                                tile = jnp.where(sub < SUB // 2, low, pltpu.roll(high, SUB // 2, 0))
                            else:
                                tile = jnp.where(sub < SUB // 2, pltpu.roll(low, SUB // 2, 0), high)
                            s_ref[at, 2 * i + parity] = tile + init_ref[at]

    bufs = (x0, x1)
    for k in range(1, APPS + 1):
        reach = HALO + 1 - k
        apply_rows(
            HALO - reach,
            half + 2 * reach,
            steps,
            bufs[k % 2],
            bufs[(k + 1) % 2],
            s_ref,
            c_ref,
            p_ref,
            0,
            0,
            k == 1,
        )
    final = bufs[(APPS + 1) % 2]
    reach = HALO + 1 - APPS
    start = HALO - reach

    def out_body(i, carry):
        for n in range(steps):
            x_out[i, n] = final[start + i, n]
        return carry

    lax.fori_loop(0, half + 2 * reach, out_body, 0)

    def out_source(i, carry):
        for n in range(steps):
            s_out[i, n] = s_ref[start + 1 + i, n]
        last_out[i] = final[start + 1 + i, steps - 1]
        return carry

    lax.fori_loop(0, half + 2 * (reach - 1), out_source, 0)


def second_kernel(rows, steps, ints, floats, x_ref, s_ref, last_ref, other_ref, coef_ref, *refs):
    keep_near, keep_far, send_near, send_far = refs[:4]
    c_ref, p_ref, s0_ref, xa, xb = refs[4:]
    core, side = ints[0], ints[1]
    wrap = floats[0]
    half = rows // 2
    own = half * core
    reach = HALO - APPS
    window = half + 2 * reach
    margin = (coef_ref.shape[0] - rows) // 2

    def coef_body(i, carry):
        prepare_coefs(coef_ref, own + margin - reach + i, c_ref, p_ref, i, wrap, steps)
        for n in range(steps):
            s0_ref[i, n] = s_ref[i, n]
        s0_ref[i, 0] = s_ref[i, 0] - (0.5 * wrap) * (last_ref[i] - other_ref[i])
        return carry

    lax.fori_loop(0, window, coef_body, 0)

    bufs = [x_ref, xa]
    src, dst = x_ref, xa
    for k in range(1, APPS + 1):
        left = reach + 1 - k
        apply_rows(
            1 + reach - left, half + 2 * left, steps, src, dst, s0_ref, c_ref, p_ref, 1, 1, False
        )
        src, dst = dst, (xb if dst is xa else xa)
    sub = lax.broadcasted_iota(jnp.int32, (SUB, LANES), 0)
    for pair in range(half // 2):
        for i in range(steps // 2):
            for to_core, near, far in ((0, keep_near, keep_far), (1, send_near, send_far)):
                parity = core if to_core == 0 else 1 - core
                a = src[1 + reach + 2 * pair, 2 * i + parity]
                b = src[1 + reach + 2 * pair + 1, 2 * i + parity]
                low = jnp.where(sub < SUB // 2, a, pltpu.roll(b, SUB // 2, 0))
                high = jnp.where(sub < SUB // 2, pltpu.roll(a, SUB // 2, 0), b)
                near[i, pair] = jnp.where(side == 0, low, high)
                far[i, pair] = jnp.where(side == 0, high, low)


def banded_body(forcing, initial, coupling, velocity):
    f32 = jnp.float32
    groups = lax.axis_size("tm")
    sites = groups // 2
    steps = groups // 2
    planes, height, width = initial.shape
    rows = height // sites
    half = rows // 2
    time_index = lax.axis_index("tm")
    side = lax.axis_index("space")
    core = time_index % 2
    site = time_index // 2
    place = position(site)
    root = math.sqrt(wrap_alpha)
    wrap = jnp.where(side == 0, root, -root).astype(f32)
    ints = jnp.stack([core, side]).astype(jnp.int32)
    floats = wrap[None]

    same_core = [[2 * i + c for i in range(sites)] for c in range(2)]
    cores = [(i, i ^ 1) for i in range(groups)]
    sides = [(0, 1), (1, 0)]
    by_place = {position(q): q for q in range(sites)}
    ahead = [
        (2 * by_place[p] + c, 2 * by_place[p + 1] + c) for p in range(sites - 1) for c in range(2)
    ]
    back = [(b, a) for a, b in ahead]

    margin = HALO + 1
    margin = -(-(2 * margin + rows) // SUB) * SUB
    margin = (margin - rows) // 2
    fields = jnp.concatenate([coupling[None], velocity, initial[None]], axis=0)
    padded = jnp.pad(fields, ((0, 0), (0, 0), (margin, margin), (0, 0)))
    mine = lax.dynamic_slice_in_dim(padded, place * rows, rows + 2 * margin, axis=2)
    theirs = lax.ppermute(mine, "space", sides)

    packed = vmem_call(
        functools.partial(pack_kernel, sites, rows),
        jax.ShapeDtypeStruct((sites * (rows + 2) * planes, width), f32),
        1,
        name="pack",
    )(forcing[0])
    packed = packed.reshape(sites, (rows + 2) // 2, 2 * planes, width)
    bands = lax.all_to_all(
        packed, "tm", split_axis=0, concat_axis=0, tiled=True, axis_index_groups=same_core
    )
    near, far = bands[: steps // 2], bands[steps // 2 :]
    keep = near + wrap * far
    send = near - wrap * far
    got = lax.ppermute(send, "space", sides)

    pieces = []
    for keep_b, got_b in (
        (keep, got),
        (lax.ppermute(keep, "tm", ahead), lax.ppermute(got, "tm", ahead)),
        (lax.ppermute(keep, "tm", back), lax.ppermute(got, "tm", back)),
    ):
        pieces += [keep_b, got_b, lax.ppermute(keep_b, "tm", cores), lax.ppermute(got_b, "tm", cores)]

    halves = jnp.where(side == 0, mine, theirs), jnp.where(side == 0, theirs, mine)
    coefs = jnp.concatenate(halves, axis=1).transpose(2, 0, 1, 3)

    depth = 2 * planes
    window = half + 2 * HALO
    reach = HALO + 1 - APPS
    limit = 48 * 1024 * 1024
    tile = (depth, width)
    x_mid, s_mid, last = vmem_call(
        functools.partial(first_kernel, rows, steps),
        [
            jax.ShapeDtypeStruct((half + 2 * reach, steps) + tile, f32),
            jax.ShapeDtypeStruct((half + 2 * reach - 2, steps) + tile, f32),
            jax.ShapeDtypeStruct((half + 2 * reach - 2,) + tile, f32),
        ],
        13,
        scratch=[
            pltpu.VMEM((window, steps) + tile, f32),
            pltpu.VMEM((window, 7) + tile, f32),
            pltpu.VMEM((window, steps) + tile, f32),
            pltpu.VMEM((window, steps) + tile, f32),
            pltpu.VMEM((window, steps) + tile, f32),
            pltpu.VMEM((window,) + tile, f32),
        ],
        n_smem=2,
        flops=20_000_000,
        limit=limit,
        name="first",
    )(ints, floats, *pieces, coefs)
    other = lax.ppermute(last, "space", sides)
    quarter = jax.ShapeDtypeStruct((steps // 2, half // 2, depth, width), f32)
    keep_near, keep_far, send_near, send_far = vmem_call(
        functools.partial(second_kernel, rows, steps),
        [quarter] * 4,
        5,
        scratch=[
            pltpu.VMEM((half + 2 * reach - 2, 7) + tile, f32),
            pltpu.VMEM((half + 2 * reach - 2, steps) + tile, f32),
            pltpu.VMEM((half + 2 * reach - 2, steps) + tile, f32),
            pltpu.VMEM((half + 2 * reach, steps) + tile, f32),
            pltpu.VMEM((half + 2 * reach, steps) + tile, f32),
        ],
        n_smem=2,
        flops=10_000_000,
        limit=limit,
        name="second",
    )(ints, floats, x_mid, s_mid, last, other, coefs)

    got_near = lax.ppermute(send_near, "tm", cores)
    got_far = lax.ppermute(send_far, "tm", cores)
    mate_near = lax.ppermute(keep_far, "space", sides)
    mate_far = lax.ppermute(got_far, "space", sides)
    ours = jnp.stack([keep_near, got_near], axis=1)
    mates = jnp.stack([mate_near, mate_far], axis=1)
    early = 0.5 * (ours + mates)
    late = (0.5 / (wrap)) * (ours - mates)
    result = jnp.concatenate([early, late], axis=0)
    spread = lax.all_to_all(
        result, "tm", split_axis=0, concat_axis=0, tiled=True, axis_index_groups=same_core
    )
    return vmem_call(
        functools.partial(unpack_kernel, sites, rows),
        jax.ShapeDtypeStruct((1, planes, height, width), f32),
        2,
        n_smem=1,
        name="unpack",
    )(ints, spread.reshape(-1, width), initial)


def passed_along(array, axis, by):
    size = lax.axis_size(axis)
    pairs = [(i, i + by) for i in range(size) if 0 <= i + by < size]
    return lax.ppermute(array, axis, pairs)


def with_halo(block, sides, width):
    for axis, dim in sides:
        count = lax.axis_size(axis)
        forward = [(i, i + 1) for i in range(count - 1)]
        backward = [(target, source) for source, target in forward]
        low = lax.ppermute(
            lax.slice_in_dim(block, block.shape[dim] - width, None, axis=dim), axis, forward
        )
        high = lax.ppermute(lax.slice_in_dim(block, 0, width, axis=dim), axis, backward)
        block = jnp.concatenate([low, block, high], axis=dim)
    return block


def coupled(extended, coupling, advect):
    total = (coupling - advect[0]) * extended[..., 2:, 1:-1, 1:-1] + (
        coupling + advect[0]
    ) * extended[..., :-2, 1:-1, 1:-1]
    total = (
        total
        + (coupling - advect[1]) * extended[..., 1:-1, 2:, 1:-1]
        + (coupling + advect[1]) * extended[..., 1:-1, :-2, 1:-1]
    )
    total = (
        total
        + (coupling - advect[2]) * extended[..., 1:-1, 1:-1, 2:]
        + (coupling + advect[2]) * extended[..., 1:-1, 1:-1, :-2]
    )
    return total


def tables(total_steps):
    indices = jnp.arange(total_steps, dtype=jnp.int32)
    products = indices[:, None] * indices[None, :] % total_steps
    angles = products.astype(jnp.float32) * (2.0 * math.pi / total_steps)
    return (jnp.cos(angles), jnp.sin(angles))


def matmul(table, columns):
    return jnp.dot(
        table, columns, preferred_element_type=jnp.float32, precision=lax.Precision.HIGHEST
    )


def jacobi(spectrum, coupling, advect, frequency, total_steps, extend):
    radius = math.exp(math.log(wrap_alpha) / total_steps)
    angles = (frequency * (2.0 * math.pi / total_steps))[:, None, None, None]
    diag_re = 1.0 + 6.0 * coupling - radius * jnp.cos(angles)
    diag_im = radius * jnp.sin(angles) + jnp.zeros_like(diag_re)
    modulus = diag_re * diag_re + diag_im * diag_im
    source_re = spectrum[0]
    source_im = spectrum[1]
    value_re = (source_re * diag_re + source_im * diag_im) / modulus
    value_im = (source_im * diag_re - source_re * diag_im) / modulus
    for sweep in range(SWEEPS):
        extended = extend(jnp.stack([value_re, value_im]))
        summed = coupled(extended, coupling, advect)
        sum_re = source_re + summed[0]
        sum_im = source_im + summed[1]
        value_re = (sum_re * diag_re + sum_im * diag_im) / modulus
        value_im = (sum_im * diag_re - sum_re * diag_im) / modulus
    return jnp.stack([value_re, value_im])


def general_body(forcing, initial, coupling, velocity):
    local_steps = forcing.shape[0]
    groups = lax.axis_size("tm")
    total_steps = local_steps * groups
    time_index = lax.axis_index("tm")
    advect = coupling[None] * velocity
    cosine, sine_table = tables(total_steps)
    global_steps = (time_index * local_steps + jnp.arange(local_steps, dtype=jnp.int32)).astype(
        jnp.float32
    )
    time_weight = jnp.exp(math.log(wrap_alpha) * global_steps / total_steps)[:, None, None, None]
    iterate = jnp.broadcast_to(initial, forcing.shape)

    def forward(piece):
        columns = piece.reshape(piece.shape[0], -1)
        spec_re = matmul(cosine, columns)
        spec_im = -matmul(sine_table, columns)
        return jnp.stack([spec_re, spec_im]).reshape((2,) + piece.shape)

    for repeat in range(ITERS):
        before = passed_along(iterate[-1], "tm", 1)
        before = jnp.where(time_index == 0, initial, before)
        previous = jnp.concatenate([before[None], iterate[:-1]], axis=0)
        extended = with_halo(iterate, (("space", 1),), 1)
        extended = jnp.pad(extended, ((0, 0), (0, 0), (1, 1), (1, 1)))
        residual = (
            forcing
            - ((1.0 + 6.0 * coupling) * iterate - coupled(extended, coupling, advect))
            + previous
        )
        scaled = residual * time_weight
        spectrum = forward(lax.all_to_all(scaled, "tm", split_axis=2, concat_axis=0, tiled=True))
        blocked = lax.all_to_all(spectrum, "tm", split_axis=1, concat_axis=3, tiled=True)
        frequency = (time_index * local_steps + jnp.arange(local_steps, dtype=jnp.int32)).astype(
            jnp.float32
        )

        def extend_narrow(field):
            grown = with_halo(field, (("space", 2),), 1)
            return jnp.pad(grown, ((0, 0), (0, 0), (0, 0), (1, 1), (1, 1)))

        solved = jacobi(blocked, coupling, advect, frequency, total_steps, extend_narrow)
        spectrum_out = lax.all_to_all(solved, "tm", split_axis=3, concat_axis=1, tiled=True)
        inverse_part = (
            matmul(cosine, spectrum_out[0].reshape(total_steps, -1))
            - matmul(sine_table, spectrum_out[1].reshape(total_steps, -1))
        ) / total_steps
        inverse_part = inverse_part.reshape(spectrum_out.shape[1:])
        correction = lax.all_to_all(inverse_part, "tm", split_axis=0, concat_axis=2, tiled=True)
        iterate = iterate + correction / time_weight
    return iterate


def body(forcing, initial, coupling, velocity):
    groups = lax.axis_size("tm")
    planes, height, width = initial.shape
    fits = (
        ITERS == 2
        and forcing.shape[0] == 1
        and groups % 4 == 0
        and lax.axis_size("space") == 2
        and 2 * planes == SUB
        and width == LANES
        and height % (groups * SUB) == 0
        and height // (groups // 2) + 1 >= HALO
    )
    plan = banded_body if fits else general_body
    return plan(forcing, initial, coupling, velocity)


def solution(mesh):
    return jax.shard_map(
        body,
        mesh=mesh,
        in_specs=(
            P("tm", "space", None, None),
            P("space", None, None),
            P("space", None, None),
            P(None, "space", None, None),
        ),
        out_specs=P("tm", "space", None, None),
        check_vma=False,
    )
```

```python
import functools
import math

import jax
import jax.numpy as jnp
from jax import lax
from jax.experimental import pallas as pl
from jax.experimental.pallas import tpu as pltpu
from jax.sharding import PartitionSpec as P

ITERS = 2
SWEEPS = 8

wrap_alpha = 0.1

APPS = SWEEPS + 1
HALO = ITERS * APPS - 1
GROUP = 6
PREPARED = 4
LANES = 128
SUB = 8


def position(site):
    a, b = site // 2, site % 2
    return 2 * a + (b ^ (a % 2))


def vmem_call(kernel, out_shapes, n_in, scratch=(), n_smem=0, flops=0, limit=8 << 20, name=None, flags=None):
    specs = [pl.BlockSpec(memory_space=pltpu.SMEM)] * n_smem
    specs += [pl.BlockSpec(memory_space=pltpu.VMEM)] * n_in
    multi = isinstance(out_shapes, (tuple, list))
    outs = pl.BlockSpec(memory_space=pltpu.VMEM)
    return pl.pallas_call(
        kernel,
        out_shape=out_shapes,
        in_specs=specs,
        out_specs=[outs] * len(out_shapes) if multi else outs,
        scratch_shapes=list(scratch),
        compiler_params=pltpu.CompilerParams(vmem_limit_bytes=limit, flags=flags),
        cost_estimate=pl.CostEstimate(flops=flops, bytes_accessed=1 << 20, transcendentals=0),
        name=name,
    )


def pack_kernel(sites, rows, f_ref, o_ref):
    planes, total = f_ref.shape[0], f_ref.shape[1]
    block = (rows + 2) * planes
    for site in range(sites):
        first = position(site) * rows
        base = site * block
        for z in range(planes):
            for part in range(rows // SUB):
                tile = f_ref[z, pl.ds(first + part * SUB, SUB), :]
                o_ref[pl.ds(base + (1 + part * SUB) * planes + z, SUB, stride=planes), :] = tile
            for idx, row in ((0, first - 1), (rows + 1, first + rows)):
                if 0 <= row < total:
                    edge = f_ref[z, pl.ds(row, 1), :]
                else:
                    edge = jnp.zeros((1, LANES), jnp.float32)
                o_ref[pl.ds(base + idx * planes + z, 1), :] = edge


def unpack_kernel(sites, rows, ints, r_ref, i_ref, o_ref):
    core = ints[0]
    planes = i_ref.shape[0]
    half = rows // 2
    for site in range(sites):
        first = position(site) * rows
        for part in range(2):
            who = core if part == 0 else 1 - core
            base = (site * 2 + part) * half * planes
            for z in range(planes):
                for piece in range(half // SUB):
                    row = pl.multiple_of(first + who * half + piece * SUB, SUB)
                    tile = r_ref[pl.ds(base + piece * SUB * planes + z, SUB, stride=planes), :]
                    o_ref[0, z, pl.ds(row, SUB), :] = i_ref[z, pl.ds(row, SUB), :] + tile


def shifts(mid, low, high, left, right, coefs):
    depth = mid.shape[0]
    zp, zm, yp, ym, xp, xm = coefs
    out = zp * pltpu.roll(mid, depth - 1, 0) + zm * pltpu.roll(mid, 1, 0)
    out = out + (yp * high + ym * low)
    return out + (xp * left + xm * right)


def moved(mid):
    return pltpu.roll(mid, LANES - 1, 1), pltpu.roll(mid, 1, 1)


def merge_kernel(ints, keep_ref, got_ref, o_ref):
    side = ints[1]
    sub = lax.broadcasted_iota(jnp.int32, (SUB, LANES), 0)
    for i in range(keep_ref.shape[0]):
        for pair in range(keep_ref.shape[1]):
            a, b = keep_ref[i, pair], got_ref[i, pair]
            low = jnp.where(side == 0, a, b)
            high = jnp.where(side == 0, b, a)
            o_ref[2 * pair, i] = jnp.where(sub < SUB // 2, low, pltpu.roll(high, SUB // 2, 0))
            o_ref[2 * pair + 1, i] = jnp.where(sub < SUB // 2, pltpu.roll(low, SUB // 2, 0), high)


def prepare_kernel(steps, skip, floats, coef_ref, c_ref, p_ref, g_ref):
    wrap = floats[0]
    count = c_ref.shape[0]
    tile = coef_ref.shape[2:]
    z = lax.broadcasted_iota(jnp.int32, tile, 0)
    x = lax.broadcasted_iota(jnp.int32, tile, 1)

    def group_body(i, carry):
        states = [coef_ref[i * PREPARED + skip + u, 4] for u in range(PREPARED)]
        sides = [moved(state) for state in states]
        for u in range(PREPARED):
            row = i * PREPARED + u
            at = row + skip
            coupling = coef_ref[at, 0]
            coefs = []
            for k in range(3):
                advect = coupling * coef_ref[at, 1 + k]
                plus, minus = coupling - advect, coupling + advect
                if k == 0:
                    plus = jnp.where(z == tile[0] - 1, 0.0, plus)
                    minus = jnp.where(z == 0, 0.0, minus)
                if k == 2:
                    plus = jnp.where(x == LANES - 1, 0.0, plus)
                    minus = jnp.where(x == 0, 0.0, minus)
                coefs += [plus, minus]
            inv = 1.0 / (1.0 + 6.0 * coupling)
            for k, value in enumerate(coefs + [inv]):
                c_ref[row, k] = value
            powers = [inv]
            for _ in range(steps - 1):
                powers.append(powers[-1] * inv)
            scale = wrap / (1.0 - wrap * powers[-1])
            for n in range(steps):
                p_ref[row, n] = scale * powers[n]
            around = shifts(states[u], coef_ref[at - 1, 4], coef_ref[at + 1, 4], *sides[u], coefs)
            g_ref[row] = (around - 6.0 * coupling * states[u]) * (1.0 + wrap)
        return carry

    lax.fori_loop(0, count // PREPARED, group_body, 0)


def apply_rows(lo, base, count, steps, src, dst, move, side_ref, s_ref, c_ref, p_ref, more, then, fix):
    groups = -(-count // GROUP)

    def solve(r):
        for u in range(GROUP):
            at = r + u + base
            coefs = [c_ref[at, k] for k in range(6)]
            inv = c_ref[at, 6]
            run = None
            ys = []
            for n in range(steps):
                b = s_ref[at, n]
                if n == 0 and fix is not None:
                    b = b - fix(r + u)
                if more:
                    b = b + shifts(
                        src[r + u, n],
                        src[r + u - 1, n],
                        src[r + u + 1, n],
                        side_ref[u, n, 0],
                        side_ref[u, n, 1],
                        coefs,
                    )
                run = b * inv if run is None else (b + run) * inv
                ys.append(run)
            for n in range(steps):
                dst[r + u - move, n] = ys[n] + ys[-1] * p_ref[at, n]

    def group_body(i, carry):
        r = lo + i * GROUP
        coming = take_sides(src, r + GROUP, steps) if more else None
        solve(r)
        if more:
            put_sides(side_ref, coming, steps)
        return carry

    lax.fori_loop(0, groups - 1, group_body, 0)
    early = then is not None and groups > 2
    coming = take_sides(dst, then, steps) if early else None
    solve(lo + (groups - 1) * GROUP)
    if then is not None:
        put_sides(side_ref, coming if early else take_sides(dst, then, steps), steps)


def take_sides(ref, r, steps):
    return [[moved(ref[r + u, n]) for n in range(steps)] for u in range(GROUP)]


def put_sides(side_ref, values, steps):
    for u in range(GROUP):
        for n in range(steps):
            side_ref[u, n, 0], side_ref[u, n, 1] = values[u][n]


def first_kernel(rows, steps, ints, *refs):
    bands, (c_ref, p_ref, g_ref) = refs[:6], refs[6:9]
    x_out, s_ref, last_out = refs[9:12]
    x0, x1, side_ref = refs[12:]
    core = ints[0]
    half = rows // 2
    own = half * core

    for band, skip, first, count in ((0, 1, HALO, rows), (1, 0, 0, HALO), (2, 1, HALO + rows, HALO)):
        for who in range(2):
            band_ref = bands[2 * band + who]
            parity = core if who == 0 else 1 - core
            skipped = rows + 1 - HALO if band == 1 else skip
            for j in range(count):
                for i in range(steps // 2):
                    value = band_ref[skipped + j, i] + g_ref[first + j]
                    s_ref[first + j, 2 * i + parity] = value
    for row in range(2 * HALO + rows, s_ref.shape[0]):
        for n in range(steps):
            s_ref[row, n] = jnp.zeros_like(g_ref[0])

    bufs = (x0, x1)
    for k in range(1, APPS + 1):
        reach = HALO + 1 - k
        final = k == APPS
        apply_rows(
            own + HALO - reach,
            0,
            half + 2 * reach,
            steps,
            bufs[k % 2],
            x_out if final else bufs[(k + 1) % 2],
            own + HALO - reach if final else 0,
            side_ref,
            s_ref,
            c_ref,
            p_ref,
            k > 1,
            None if final else own + HALO - reach + 1,
            None,
        )
    for i in range(last_out.shape[0]):
        last_out[i] = x_out[i + 1, steps - 1]


def second_kernel(rows, steps, ints, floats, x_ref, s_ref, last_ref, other_ref, c_ref, p_ref, *refs):
    keep_near, keep_far, send_near, send_far = refs[:4]
    xa, xb, side_ref = refs[4:]
    core, side = ints[0], ints[1]
    wrap = floats[0]
    half = rows // 2
    reach = HALO - APPS
    base = half * core + HALO - reach - 1

    def fix(r):
        return (0.5 * wrap) * (last_ref[r - 1] - other_ref[r - 1])

    src, dst = x_ref, xa
    put_sides(side_ref, take_sides(x_ref, 1, steps), steps)
    for k in range(1, APPS + 1):
        left = reach + 1 - k
        lo = 1 + reach - left
        then = lo + 1 if k < APPS else None
        apply_rows(
            lo, base, half + 2 * left, steps, src, dst, 0, side_ref, s_ref, c_ref, p_ref, True, then, fix
        )
        src, dst = dst, (xb if dst is xa else xa)
    sub = lax.broadcasted_iota(jnp.int32, (SUB, LANES), 0)
    for pair in range(half // 2):
        for i in range(steps // 2):
            for to_core, near, far in ((0, keep_near, keep_far), (1, send_near, send_far)):
                parity = core if to_core == 0 else 1 - core
                a = src[1 + reach + 2 * pair, 2 * i + parity]
                b = src[1 + reach + 2 * pair + 1, 2 * i + parity]
                low = jnp.where(sub < SUB // 2, a, pltpu.roll(b, SUB // 2, 0))
                high = jnp.where(sub < SUB // 2, pltpu.roll(a, SUB // 2, 0), b)
                near[i, pair] = jnp.where(side == 0, low, high)
                far[i, pair] = jnp.where(side == 0, high, low)


def banded_body(forcing, initial, coupling, velocity):
    f32 = jnp.float32
    groups = lax.axis_size("tm")
    sites = groups // 2
    steps = groups // 2
    planes, height, width = initial.shape
    rows = height // sites
    half = rows // 2
    depth = 2 * planes
    tile = (depth, width)
    time_index = lax.axis_index("tm")
    side = lax.axis_index("space")
    core = time_index % 2
    site = time_index // 2
    place = position(site)
    root = math.sqrt(wrap_alpha)
    wrap = jnp.where(side == 0, root, -root).astype(f32)
    ints = jnp.stack([core, side]).astype(jnp.int32)
    floats = wrap[None]

    same_core = [[2 * i + c for i in range(sites)] for c in range(2)]
    cores = [(i, i ^ 1) for i in range(groups)]
    sides = [(0, 1), (1, 0)]
    by_place = {position(q): q for q in range(sites)}
    ahead = [
        (2 * by_place[p] + c, 2 * by_place[p + 1] + c) for p in range(sites - 1) for c in range(2)
    ]
    back = [(b, a) for a, b in ahead]

    window = -(-(rows + 2 * HALO) // PREPARED) * PREPARED
    margin = HALO + 1
    margin = (-(-(rows + 2 * margin) // SUB) * SUB - rows) // 2
    fields = jnp.concatenate([coupling[None], velocity, initial[None]], axis=0)
    padded = jnp.pad(fields, ((0, 0), (0, 0), (margin, margin), (0, 0)))
    mine = lax.dynamic_slice_in_dim(padded, place * rows, rows + 2 * margin, axis=2)
    share = lax.dynamic_slice_in_dim(mine, core * (planes // 2), planes // 2, axis=1)
    share = lax.ppermute(share, "space", sides)
    packed = vmem_call(
        functools.partial(pack_kernel, sites, rows),
        jax.ShapeDtypeStruct((sites * (rows + 2) * planes, width), f32),
        1,
        name="pack",
    )(forcing[0])
    packed = packed.reshape(sites, (rows + 2) // 2, 2 * planes, width)
    arrived = lax.all_to_all(
        packed, "tm", split_axis=0, concat_axis=0, tiled=True, axis_index_groups=same_core
    )
    near, far = arrived[: steps // 2], arrived[steps // 2 :]
    keep = near + wrap * far
    send = near - wrap * far
    got = lax.ppermute(send, "space", sides)
    got, share = lax.optimization_barrier((got, share))
    mate_share = lax.ppermute(share, "tm", cores)
    band = vmem_call(
        merge_kernel,
        jax.ShapeDtypeStruct((rows + 2, steps // 2) + tile, f32),
        2,
        n_smem=1,
        name="merge",
    )(ints, keep, got)
    ahead_band = lax.ppermute(band, "tm", ahead)
    back_band = lax.ppermute(band, "tm", back)

    low, high = jnp.where(core == 0, share, mate_share), jnp.where(core == 0, mate_share, share)
    theirs = jnp.concatenate([low, high], axis=1)
    halves = jnp.where(side == 0, mine, theirs), jnp.where(side == 0, theirs, mine)
    coefs = jnp.concatenate(halves, axis=1).transpose(2, 0, 1, 3)
    weights, wraps, extra = vmem_call(
        functools.partial(prepare_kernel, steps, margin - HALO),
        [
            jax.ShapeDtypeStruct((window, 7) + tile, f32),
            jax.ShapeDtypeStruct((window, steps) + tile, f32),
            jax.ShapeDtypeStruct((window,) + tile, f32),
        ],
        1,
        n_smem=1,
        flops=5_000_000,
        name="prepare",
    )(floats, coefs)

    ahead_band, weights, wraps, extra = lax.optimization_barrier(
        (ahead_band, weights, wraps, extra)
    )
    bands = []
    for each in (band, ahead_band, back_band):
        bands += [each, lax.ppermute(each, "tm", cores)]

    reach = HALO + 1 - APPS
    limit = 12 * 1024 * 1024
    spare = GROUP
    x_mid, source, last = vmem_call(
        functools.partial(first_kernel, rows, steps),
        [
            jax.ShapeDtypeStruct((half + 2 * reach + spare, steps) + tile, f32),
            jax.ShapeDtypeStruct((window, steps) + tile, f32),
            jax.ShapeDtypeStruct((half + 2 * reach + GROUP - 3,) + tile, f32),
        ],
        9,
        scratch=[
            pltpu.VMEM((window + spare, steps) + tile, f32),
            pltpu.VMEM((window + spare, steps) + tile, f32),
            pltpu.VMEM((GROUP, steps, 2) + tile, f32),
        ],
        n_smem=1,
        flops=20_000_000,
        limit=limit,
        name="first",
    )(ints, *bands, weights, wraps, extra)
    other = lax.ppermute(last, "space", sides)
    quarter = jax.ShapeDtypeStruct((steps // 2, half // 2) + tile, f32)
    keep_near, keep_far, send_near, send_far = vmem_call(
        functools.partial(second_kernel, rows, steps),
        [quarter] * 4,
        6,
        scratch=[
            pltpu.VMEM((half + 2 * reach + spare, steps) + tile, f32),
            pltpu.VMEM((half + 2 * reach + spare, steps) + tile, f32),
            pltpu.VMEM((GROUP, steps, 2) + tile, f32),
        ],
        n_smem=2,
        flops=10_000_000,
        limit=limit,
        name="second",
    )(ints, floats, x_mid, source, last, other, weights, wraps)

    got_near = lax.ppermute(send_near, "tm", cores)
    got_far = lax.ppermute(send_far, "tm", cores)
    mate_near = lax.ppermute(keep_far, "space", sides)
    mate_far = lax.ppermute(got_far, "space", sides)
    ours = jnp.stack([keep_near, got_near], axis=1)
    mates = jnp.stack([mate_near, mate_far], axis=1)
    early = 0.5 * (ours + mates)
    late = (0.5 / wrap) * (ours - mates)
    result = jnp.concatenate([early, late], axis=0)
    spread = lax.all_to_all(
        result, "tm", split_axis=0, concat_axis=0, tiled=True, axis_index_groups=same_core
    )
    return vmem_call(
        functools.partial(unpack_kernel, sites, rows),
        jax.ShapeDtypeStruct((1, planes, height, width), f32),
        2,
        n_smem=1,
        name="unpack",
    )(ints, spread.reshape(-1, width), initial)


def passed_along(array, axis, by):
    size = lax.axis_size(axis)
    pairs = [(i, i + by) for i in range(size) if 0 <= i + by < size]
    return lax.ppermute(array, axis, pairs)


def with_halo(block, sides, width):
    for axis, dim in sides:
        count = lax.axis_size(axis)
        forward = [(i, i + 1) for i in range(count - 1)]
        backward = [(target, source) for source, target in forward]
        low = lax.ppermute(
            lax.slice_in_dim(block, block.shape[dim] - width, None, axis=dim), axis, forward
        )
        high = lax.ppermute(lax.slice_in_dim(block, 0, width, axis=dim), axis, backward)
        block = jnp.concatenate([low, block, high], axis=dim)
    return block


def coupled(extended, coupling, advect):
    total = (coupling - advect[0]) * extended[..., 2:, 1:-1, 1:-1] + (
        coupling + advect[0]
    ) * extended[..., :-2, 1:-1, 1:-1]
    total = (
        total
        + (coupling - advect[1]) * extended[..., 1:-1, 2:, 1:-1]
        + (coupling + advect[1]) * extended[..., 1:-1, :-2, 1:-1]
    )
    total = (
        total
        + (coupling - advect[2]) * extended[..., 1:-1, 1:-1, 2:]
        + (coupling + advect[2]) * extended[..., 1:-1, 1:-1, :-2]
    )
    return total


def tables(total_steps):
    indices = jnp.arange(total_steps, dtype=jnp.int32)
    products = indices[:, None] * indices[None, :] % total_steps
    angles = products.astype(jnp.float32) * (2.0 * math.pi / total_steps)
    return (jnp.cos(angles), jnp.sin(angles))


def matmul(table, columns):
    return jnp.dot(
        table, columns, preferred_element_type=jnp.float32, precision=lax.Precision.HIGHEST
    )


def jacobi(spectrum, coupling, advect, frequency, total_steps, extend):
    radius = math.exp(math.log(wrap_alpha) / total_steps)
    angles = (frequency * (2.0 * math.pi / total_steps))[:, None, None, None]
    diag_re = 1.0 + 6.0 * coupling - radius * jnp.cos(angles)
    diag_im = radius * jnp.sin(angles) + jnp.zeros_like(diag_re)
    modulus = diag_re * diag_re + diag_im * diag_im
    source_re = spectrum[0]
    source_im = spectrum[1]
    value_re = (source_re * diag_re + source_im * diag_im) / modulus
    value_im = (source_im * diag_re - source_re * diag_im) / modulus
    for sweep in range(SWEEPS):
        extended = extend(jnp.stack([value_re, value_im]))
        summed = coupled(extended, coupling, advect)
        sum_re = source_re + summed[0]
        sum_im = source_im + summed[1]
        value_re = (sum_re * diag_re + sum_im * diag_im) / modulus
        value_im = (sum_im * diag_re - sum_re * diag_im) / modulus
    return jnp.stack([value_re, value_im])


def general_body(forcing, initial, coupling, velocity):
    local_steps = forcing.shape[0]
    groups = lax.axis_size("tm")
    total_steps = local_steps * groups
    time_index = lax.axis_index("tm")
    advect = coupling[None] * velocity
    cosine, sine_table = tables(total_steps)
    global_steps = (time_index * local_steps + jnp.arange(local_steps, dtype=jnp.int32)).astype(
        jnp.float32
    )
    time_weight = jnp.exp(math.log(wrap_alpha) * global_steps / total_steps)[:, None, None, None]
    iterate = jnp.broadcast_to(initial, forcing.shape)

    def forward(piece):
        columns = piece.reshape(piece.shape[0], -1)
        spec_re = matmul(cosine, columns)
        spec_im = -matmul(sine_table, columns)
        return jnp.stack([spec_re, spec_im]).reshape((2,) + piece.shape)

    for repeat in range(ITERS):
        before = passed_along(iterate[-1], "tm", 1)
        before = jnp.where(time_index == 0, initial, before)
        previous = jnp.concatenate([before[None], iterate[:-1]], axis=0)
        extended = with_halo(iterate, (("space", 1),), 1)
        extended = jnp.pad(extended, ((0, 0), (0, 0), (1, 1), (1, 1)))
        residual = (
            forcing
            - ((1.0 + 6.0 * coupling) * iterate - coupled(extended, coupling, advect))
            + previous
        )
        scaled = residual * time_weight
        spectrum = forward(lax.all_to_all(scaled, "tm", split_axis=2, concat_axis=0, tiled=True))
        blocked = lax.all_to_all(spectrum, "tm", split_axis=1, concat_axis=3, tiled=True)
        frequency = (time_index * local_steps + jnp.arange(local_steps, dtype=jnp.int32)).astype(
            jnp.float32
        )

        def extend_narrow(field):
            grown = with_halo(field, (("space", 2),), 1)
            return jnp.pad(grown, ((0, 0), (0, 0), (0, 0), (1, 1), (1, 1)))

        solved = jacobi(blocked, coupling, advect, frequency, total_steps, extend_narrow)
        spectrum_out = lax.all_to_all(solved, "tm", split_axis=3, concat_axis=1, tiled=True)
        inverse_part = (
            matmul(cosine, spectrum_out[0].reshape(total_steps, -1))
            - matmul(sine_table, spectrum_out[1].reshape(total_steps, -1))
        ) / total_steps
        inverse_part = inverse_part.reshape(spectrum_out.shape[1:])
        correction = lax.all_to_all(inverse_part, "tm", split_axis=0, concat_axis=2, tiled=True)
        iterate = iterate + correction / time_weight
    return iterate


def body(forcing, initial, coupling, velocity):
    groups = lax.axis_size("tm")
    planes, height, width = initial.shape
    fits = (
        ITERS == 2
        and forcing.shape[0] == 1
        and groups % 4 == 0
        and lax.axis_size("space") == 2
        and 2 * planes == SUB
        and width == LANES
        and height % (groups * SUB) == 0
        and height // (groups // 2) + 1 >= HALO
    )
    plan = banded_body if fits else general_body
    return plan(forcing, initial, coupling, velocity)


def solution(mesh):
    return jax.shard_map(
        body,
        mesh=mesh,
        in_specs=(
            P("tm", "space", None, None),
            P("space", None, None),
            P("space", None, None),
            P(None, "space", None, None),
        ),
        out_specs=P("tm", "space", None, None),
        check_vma=False,
    )
```

```python
import functools
import math

import jax
import jax.numpy as jnp
from jax import lax
from jax.experimental import pallas as pl
from jax.experimental.pallas import tpu as pltpu
from jax.sharding import PartitionSpec as P

ITERS = 2
SWEEPS = 8

wrap_alpha = 0.1

APPS = SWEEPS + 1
HALO = ITERS * APPS - 1
GROUP = 6
PREPARED = 4
LANES = 128
SUB = 8


def position(site):
    a, b = site // 2, site % 2
    return 2 * a + (b ^ (a % 2))


def vmem_call(kernel, out_shapes, n_in, scratch=(), n_smem=0, flops=0, limit=8 << 20):
    specs = [pl.BlockSpec(memory_space=pltpu.SMEM)] * n_smem
    specs += [pl.BlockSpec(memory_space=pltpu.VMEM)] * n_in
    multi = isinstance(out_shapes, (tuple, list))
    outs = pl.BlockSpec(memory_space=pltpu.VMEM)
    return pl.pallas_call(
        kernel,
        out_shape=out_shapes,
        in_specs=specs,
        out_specs=[outs] * len(out_shapes) if multi else outs,
        scratch_shapes=list(scratch),
        compiler_params=pltpu.CompilerParams(vmem_limit_bytes=limit),
        cost_estimate=pl.CostEstimate(flops=flops, bytes_accessed=1 << 20, transcendentals=0),
    )


def pack_kernel(sites, rows, f_ref, o_ref):
    planes, total = f_ref.shape[0], f_ref.shape[1]
    block = (rows + 2) * planes
    for site in range(sites):
        first = position(site) * rows
        base = site * block
        for z in range(planes):
            for part in range(rows // SUB):
                tile = f_ref[z, pl.ds(first + part * SUB, SUB), :]
                o_ref[pl.ds(base + (1 + part * SUB) * planes + z, SUB, stride=planes), :] = tile
            for idx, row in ((0, first - 1), (rows + 1, first + rows)):
                if 0 <= row < total:
                    edge = f_ref[z, pl.ds(row, 1), :]
                else:
                    edge = jnp.zeros((1, LANES), jnp.float32)
                o_ref[pl.ds(base + idx * planes + z, 1), :] = edge


def unpack_kernel(sites, rows, ints, r_ref, i_ref, o_ref):
    core = ints[0]
    planes = i_ref.shape[0]
    half = rows // 2
    for site in range(sites):
        first = position(site) * rows
        for part in range(2):
            who = core if part == 0 else 1 - core
            base = (site * 2 + part) * half * planes
            for z in range(planes):
                for piece in range(half // SUB):
                    row = pl.multiple_of(first + who * half + piece * SUB, SUB)
                    tile = r_ref[pl.ds(base + piece * SUB * planes + z, SUB, stride=planes), :]
                    o_ref[0, z, pl.ds(row, SUB), :] = i_ref[z, pl.ds(row, SUB), :] + tile


def shifts(mid, low, high, left, right, coefs):
    depth = mid.shape[0]
    zp, zm, yp, ym, xp, xm = coefs
    out = zp * pltpu.roll(mid, depth - 1, 0) + zm * pltpu.roll(mid, 1, 0)
    out = out + (yp * high + ym * low)
    return out + (xp * left + xm * right)


def moved(mid):
    return pltpu.roll(mid, LANES - 1, 1), pltpu.roll(mid, 1, 1)


def merge_kernel(ints, keep_ref, got_ref, share_ref, o_ref, blob_ref):
    side = ints[1]
    sub = lax.broadcasted_iota(jnp.int32, (SUB, LANES), 0)
    steps, pairs = keep_ref.shape[:2]
    for i in range(steps):
        for pair in range(pairs):
            a, b = keep_ref[i, pair], got_ref[i, pair]
            low = jnp.where(side == 0, a, b)
            high = jnp.where(side == 0, b, a)
            tiles = (
                jnp.where(sub < SUB // 2, low, pltpu.roll(high, SUB // 2, 0)),
                jnp.where(sub < SUB // 2, pltpu.roll(low, SUB // 2, 0), high),
            )
            for h in range(2):
                o_ref[2 * pair + h, i] = tiles[h]
                blob_ref[(2 * pair + h) * steps + i] = tiles[h]
    at = 2 * pairs * steps
    for field in range(share_ref.shape[0]):
        for z in range(share_ref.shape[1]):
            for piece in range(share_ref.shape[2] // SUB):
                blob_ref[at] = share_ref[field, z, pl.ds(piece * SUB, SUB), :]
                at += 1


def prepare_kernel(steps, skip, half, ints, floats, coef_ref, c_ref, p_ref, g_ref):
    wrap = floats[0]
    skip = skip + half * ints[0]
    count = c_ref.shape[0]
    tile = coef_ref.shape[2:]
    z = lax.broadcasted_iota(jnp.int32, tile, 0)
    x = lax.broadcasted_iota(jnp.int32, tile, 1)

    def group_body(i, carry):
        states = [coef_ref[i * PREPARED + skip + u, 4] for u in range(PREPARED)]
        sides = [moved(state) for state in states]
        for u in range(PREPARED):
            row = i * PREPARED + u
            at = row + skip
            coupling = coef_ref[at, 0]
            coefs = []
            for k in range(3):
                advect = coupling * coef_ref[at, 1 + k]
                plus, minus = coupling - advect, coupling + advect
                if k == 0:
                    plus = jnp.where(z == tile[0] - 1, 0.0, plus)
                    minus = jnp.where(z == 0, 0.0, minus)
                if k == 2:
                    plus = jnp.where(x == LANES - 1, 0.0, plus)
                    minus = jnp.where(x == 0, 0.0, minus)
                coefs += [plus, minus]
            inv = 1.0 / (1.0 + 6.0 * coupling)
            for k, value in enumerate(coefs + [inv]):
                c_ref[row, k] = value
            powers = [inv]
            for _ in range(steps - 1):
                powers.append(powers[-1] * inv)
            scale = wrap / (1.0 - wrap * powers[-1])
            for n in range(steps):
                p_ref[row, n] = scale * powers[n]
            around = shifts(states[u], coef_ref[at - 1, 4], coef_ref[at + 1, 4], *sides[u], coefs)
            g_ref[row] = (around - 6.0 * coupling * states[u]) * (1.0 + wrap)
        return carry

    lax.fori_loop(0, count // PREPARED, group_body, 0)


def apply_rows(lo, base, count, steps, src, dst, move, side_ref, s_ref, c_ref, p_ref, more, then, fix):
    groups = -(-count // GROUP)

    def solve(r):
        for u in range(GROUP):
            at = r + u + base
            coefs = [c_ref[at, k] for k in range(6)]
            inv = c_ref[at, 6]
            run = None
            ys = []
            for n in range(steps):
                b = s_ref[at, n]
                if n == 0 and fix is not None:
                    b = b - fix(r + u)
                if more:
                    b = b + shifts(
                        src[r + u, n],
                        src[r + u - 1, n],
                        src[r + u + 1, n],
                        side_ref[u, n, 0],
                        side_ref[u, n, 1],
                        coefs,
                    )
                run = b * inv if run is None else (b + run) * inv
                ys.append(run)
            for n in range(steps):
                dst[r + u - move, n] = ys[n] + ys[-1] * p_ref[at, n]

    def group_body(i, carry):
        r = lo + i * GROUP
        coming = take_sides(src, r + GROUP, steps) if more else None
        solve(r)
        if more:
            put_sides(side_ref, coming, steps)
        return carry

    lax.fori_loop(0, groups - 1, group_body, 0)
    early = then is not None and groups > 2
    coming = take_sides(dst, then, steps) if early else None
    solve(lo + (groups - 1) * GROUP)
    if then is not None:
        put_sides(side_ref, coming if early else take_sides(dst, then, steps), steps)


def take_sides(ref, r, steps):
    return [[moved(ref[r + u, n]) for n in range(steps)] for u in range(GROUP)]


def put_sides(side_ref, values, steps):
    for u in range(GROUP):
        for n in range(steps):
            side_ref[u, n, 0], side_ref[u, n, 1] = values[u][n]


def first_kernel(rows, steps, ints, *refs):
    band_ref, mate_ref, one_ref, mate_one_ref, two_ref, mate_two_ref = refs[:6]
    c_ref, p_ref, g_ref = refs[6:9]
    x_out, s_ref, last_out = refs[9:12]
    x0, x1, side_ref = refs[12:]
    core, odd = ints[0], ints[2]
    half = rows // 2
    skip = half * core
    per = steps // 2

    for idx in range(1, rows + 1):
        j = idx - 1 + HALO - skip
        for i in range(per):
            s_ref[j, 2 * i + core] = band_ref[idx, i] + g_ref[j]
            s_ref[j, 2 * i + 1 - core] = mate_ref[idx * per + i] + g_ref[j]

    def fill(pair, idx, j):
        for i in range(per):
            s_ref[j, 2 * i + core] = pair[0][idx, i] + g_ref[j]
            s_ref[j, 2 * i + 1 - core] = pair[1][idx, i] + g_ref[j]

    for row in range(half + 2 * HALO, s_ref.shape[0]):
        for n in range(steps):
            s_ref[row, n] = jnp.zeros_like(g_ref[0])
    tail = jnp.minimum(s_ref.shape[0] - HALO - rows + skip, rows + 1)
    for pair, previous in (((one_ref, mate_one_ref), odd), ((two_ref, mate_two_ref), 1 - odd)):

        def before(idx, carry):
            fill(pair, idx + rows + 1 - HALO, idx - skip)
            return carry

        def after(idx, carry):
            fill(pair, idx, idx - 1 + HALO + rows - skip)
            return carry

        lax.fori_loop(jnp.where(previous == 1, skip, HALO), HALO, before, 0)
        lax.fori_loop(1, jnp.where(previous == 1, 1, 1 + tail), after, 0)

    bufs = (x0, x1)
    for k in range(1, APPS + 1):
        reach = HALO + 1 - k
        final = k == APPS
        apply_rows(
            HALO - reach,
            0,
            half + 2 * reach,
            steps,
            bufs[k % 2],
            x_out if final else bufs[(k + 1) % 2],
            HALO - reach if final else 0,
            side_ref,
            s_ref,
            c_ref,
            p_ref,
            k > 1,
            None if final else HALO - reach + 1,
            None,
        )
    for i in range(last_out.shape[0]):
        last_out[i] = x_out[i + 1, steps - 1]


def second_kernel(rows, steps, ints, floats, x_ref, s_ref, last_ref, other_ref, c_ref, p_ref, *refs):
    keep_near, keep_far, send_near, send_far = refs[:4]
    xa, xb, side_ref = refs[4:]
    core, side = ints[0], ints[1]
    wrap = floats[0]
    half = rows // 2
    reach = HALO - APPS
    base = HALO - reach - 1
    count = last_ref.shape[0]

    def fix(r):
        at = jnp.minimum(r - 1, count - 1)
        return (0.5 * wrap) * (last_ref[at] - other_ref[at])

    src, dst = x_ref, xa
    put_sides(side_ref, take_sides(x_ref, 1, steps), steps)
    for k in range(1, APPS + 1):
        left = reach + 1 - k
        lo = 1 + reach - left
        then = lo + 1 if k < APPS else None
        apply_rows(
            lo, base, half + 2 * left, steps, src, dst, 0, side_ref, s_ref, c_ref, p_ref, True, then, fix
        )
        src, dst = dst, (xb if dst is xa else xa)
    sub = lax.broadcasted_iota(jnp.int32, (SUB, LANES), 0)
    for pair in range(half // 2):
        for i in range(steps // 2):
            for to_core, near, far in ((0, keep_near, keep_far), (1, send_near, send_far)):
                parity = core if to_core == 0 else 1 - core
                a = src[1 + reach + 2 * pair, 2 * i + parity]
                b = src[1 + reach + 2 * pair + 1, 2 * i + parity]
                low = jnp.where(sub < SUB // 2, a, pltpu.roll(b, SUB // 2, 0))
                high = jnp.where(sub < SUB // 2, pltpu.roll(a, SUB // 2, 0), b)
                near[i, pair] = jnp.where(side == 0, low, high)
                far[i, pair] = jnp.where(side == 0, high, low)


def banded_body(forcing, initial, coupling, velocity):
    f32 = jnp.float32
    groups = lax.axis_size("tm")
    sites = groups // 2
    steps = groups // 2
    planes, height, width = initial.shape
    rows = height // sites
    half = rows // 2
    depth = 2 * planes
    tile = (depth, width)
    time_index = lax.axis_index("tm")
    side = lax.axis_index("space")
    core = time_index % 2
    site = time_index // 2
    place = position(site)
    root = math.sqrt(wrap_alpha)
    wrap = jnp.where(side == 0, root, -root).astype(f32)
    window = -(-(half + 2 * HALO) // PREPARED) * PREPARED
    margin = (-(-(rows + 2 * (HALO + 1)) // SUB) * SUB - rows) // 2
    ints = jnp.stack([core, side, place % 2]).astype(jnp.int32)
    floats = wrap[None]

    same_core = [[2 * i + c for i in range(sites)] for c in range(2)]
    cores = [(i, i ^ 1) for i in range(groups)]
    sides = [(0, 1), (1, 0)]
    by_place = {position(q): q for q in range(sites)}

    def exchange(first):
        both = []
        for p in range(first, sites - 1, 2):
            for c in range(2):
                one, two = 2 * by_place[p] + c, 2 * by_place[p + 1] + c
                both += [(one, two), (two, one)]
        return both

    fields = jnp.concatenate([coupling[None], velocity, initial[None]], axis=0)
    padded = jnp.pad(fields, ((0, 0), (0, 0), (margin, margin), (0, 0)))
    mine = lax.dynamic_slice_in_dim(padded, place * rows, rows + 2 * margin, axis=2)
    share = lax.dynamic_slice_in_dim(mine, core * (planes // 2), planes // 2, axis=1)
    share = lax.ppermute(share, "space", sides)

    packed = vmem_call(
        functools.partial(pack_kernel, sites, rows),
        jax.ShapeDtypeStruct((sites * (rows + 2) * planes, width), f32),
        1,
    )(forcing[0])
    packed = packed.reshape(sites, (rows + 2) // 2, 2 * planes, width)
    arrived = lax.all_to_all(
        packed, "tm", split_axis=0, concat_axis=0, tiled=True, axis_index_groups=same_core
    )
    near, far = arrived[: steps // 2], arrived[steps // 2 :]
    keep = near + wrap * far
    send = near - wrap * far
    got = lax.ppermute(send, "space", sides)
    tiles = (rows + 2) * (steps // 2)
    band, blob = vmem_call(
        merge_kernel,
        [
            jax.ShapeDtypeStruct((rows + 2, steps // 2) + tile, f32),
            jax.ShapeDtypeStruct((tiles + share.size // (SUB * width), SUB, width), f32),
        ],
        3,
        n_smem=1,
    )(ints, keep, got, share)
    one = lax.ppermute(band, "tm", exchange(0))
    two = lax.ppermute(band, "tm", exchange(1))
    mate = lax.ppermute(blob, "tm", cores)
    mate_share = mate[tiles:].reshape(share.shape)

    low, high = jnp.where(core == 0, share, mate_share), jnp.where(core == 0, mate_share, share)
    theirs = jnp.concatenate([low, high], axis=1)
    halves = jnp.where(side == 0, mine, theirs), jnp.where(side == 0, theirs, mine)
    coefs = jnp.concatenate(halves, axis=1).transpose(2, 0, 1, 3)
    weights, wraps, extra = vmem_call(
        functools.partial(prepare_kernel, steps, margin - HALO, half),
        [
            jax.ShapeDtypeStruct((window, 7) + tile, f32),
            jax.ShapeDtypeStruct((window, steps) + tile, f32),
            jax.ShapeDtypeStruct((window,) + tile, f32),
        ],
        1,
        n_smem=2,
        flops=5_000_000,
    )(ints, floats, coefs)

    one, two, weights, wraps, extra = lax.optimization_barrier((one, two, weights, wraps, extra))
    mate_one = lax.ppermute(one, "tm", cores)
    mate_two = lax.ppermute(two, "tm", cores)

    reach = HALO + 1 - APPS
    limit = 12 * 1024 * 1024
    spare = GROUP
    x_mid, source, last = vmem_call(
        functools.partial(first_kernel, rows, steps),
        [
            jax.ShapeDtypeStruct((half + 2 * reach + spare, steps) + tile, f32),
            jax.ShapeDtypeStruct((window, steps) + tile, f32),
            jax.ShapeDtypeStruct((half + 2 * reach - 2,) + tile, f32),
        ],
        9,
        scratch=[
            pltpu.VMEM((window + spare, steps) + tile, f32),
            pltpu.VMEM((window + spare, steps) + tile, f32),
            pltpu.VMEM((GROUP, steps, 2) + tile, f32),
        ],
        n_smem=1,
        flops=20_000_000,
        limit=limit,
    )(ints, band, mate, one, mate_one, two, mate_two, weights, wraps, extra)
    other = lax.ppermute(last, "space", sides)
    quarter = jax.ShapeDtypeStruct((steps // 2, half // 2) + tile, f32)
    keep_near, keep_far, send_near, send_far = vmem_call(
        functools.partial(second_kernel, rows, steps),
        [quarter] * 4,
        6,
        scratch=[
            pltpu.VMEM((half + 2 * reach + spare, steps) + tile, f32),
            pltpu.VMEM((half + 2 * reach + spare, steps) + tile, f32),
            pltpu.VMEM((GROUP, steps, 2) + tile, f32),
        ],
        n_smem=2,
        flops=10_000_000,
        limit=limit,
    )(ints, floats, x_mid, source, last, other, weights, wraps)

    got_near = lax.ppermute(send_near, "tm", cores)
    got_far = lax.ppermute(send_far, "tm", cores)
    mate_near = lax.ppermute(keep_far, "space", sides)
    mate_far = lax.ppermute(got_far, "space", sides)
    ours = jnp.stack([keep_near, got_near], axis=1)
    mates = jnp.stack([mate_near, mate_far], axis=1)
    early = 0.5 * (ours + mates)
    late = (0.5 / wrap) * (ours - mates)
    result = jnp.concatenate([early, late], axis=0)
    spread = lax.all_to_all(
        result, "tm", split_axis=0, concat_axis=0, tiled=True, axis_index_groups=same_core
    )
    return vmem_call(
        functools.partial(unpack_kernel, sites, rows),
        jax.ShapeDtypeStruct((1, planes, height, width), f32),
        2,
        n_smem=1,
    )(ints, spread.reshape(-1, width), initial)


def passed_along(array, axis, by):
    size = lax.axis_size(axis)
    pairs = [(i, i + by) for i in range(size) if 0 <= i + by < size]
    return lax.ppermute(array, axis, pairs)


def with_halo(block, sides, width):
    for axis, dim in sides:
        count = lax.axis_size(axis)
        forward = [(i, i + 1) for i in range(count - 1)]
        backward = [(target, source) for source, target in forward]
        low = lax.ppermute(
            lax.slice_in_dim(block, block.shape[dim] - width, None, axis=dim), axis, forward
        )
        high = lax.ppermute(lax.slice_in_dim(block, 0, width, axis=dim), axis, backward)
        block = jnp.concatenate([low, block, high], axis=dim)
    return block


def coupled(extended, coupling, advect):
    total = (coupling - advect[0]) * extended[..., 2:, 1:-1, 1:-1] + (
        coupling + advect[0]
    ) * extended[..., :-2, 1:-1, 1:-1]
    total = (
        total
        + (coupling - advect[1]) * extended[..., 1:-1, 2:, 1:-1]
        + (coupling + advect[1]) * extended[..., 1:-1, :-2, 1:-1]
    )
    total = (
        total
        + (coupling - advect[2]) * extended[..., 1:-1, 1:-1, 2:]
        + (coupling + advect[2]) * extended[..., 1:-1, 1:-1, :-2]
    )
    return total


def tables(total_steps):
    indices = jnp.arange(total_steps, dtype=jnp.int32)
    products = indices[:, None] * indices[None, :] % total_steps
    angles = products.astype(jnp.float32) * (2.0 * math.pi / total_steps)
    return (jnp.cos(angles), jnp.sin(angles))


def matmul(table, columns):
    return jnp.dot(
        table, columns, preferred_element_type=jnp.float32, precision=lax.Precision.HIGHEST
    )


def jacobi(spectrum, coupling, advect, frequency, total_steps, extend):
    radius = math.exp(math.log(wrap_alpha) / total_steps)
    angles = (frequency * (2.0 * math.pi / total_steps))[:, None, None, None]
    diag_re = 1.0 + 6.0 * coupling - radius * jnp.cos(angles)
    diag_im = radius * jnp.sin(angles) + jnp.zeros_like(diag_re)
    modulus = diag_re * diag_re + diag_im * diag_im
    source_re = spectrum[0]
    source_im = spectrum[1]
    value_re = (source_re * diag_re + source_im * diag_im) / modulus
    value_im = (source_im * diag_re - source_re * diag_im) / modulus
    for _ in range(SWEEPS):
        extended = extend(jnp.stack([value_re, value_im]))
        summed = coupled(extended, coupling, advect)
        sum_re = source_re + summed[0]
        sum_im = source_im + summed[1]
        value_re = (sum_re * diag_re + sum_im * diag_im) / modulus
        value_im = (sum_im * diag_re - sum_re * diag_im) / modulus
    return jnp.stack([value_re, value_im])


def general_body(forcing, initial, coupling, velocity):
    local_steps = forcing.shape[0]
    groups = lax.axis_size("tm")
    total_steps = local_steps * groups
    time_index = lax.axis_index("tm")
    advect = coupling[None] * velocity
    cosine, sine_table = tables(total_steps)
    global_steps = (time_index * local_steps + jnp.arange(local_steps, dtype=jnp.int32)).astype(
        jnp.float32
    )
    time_weight = jnp.exp(math.log(wrap_alpha) * global_steps / total_steps)[:, None, None, None]
    iterate = jnp.broadcast_to(initial, forcing.shape)

    def forward(piece):
        columns = piece.reshape(piece.shape[0], -1)
        spec_re = matmul(cosine, columns)
        spec_im = -matmul(sine_table, columns)
        return jnp.stack([spec_re, spec_im]).reshape((2,) + piece.shape)

    for _ in range(ITERS):
        before = passed_along(iterate[-1], "tm", 1)
        before = jnp.where(time_index == 0, initial, before)
        previous = jnp.concatenate([before[None], iterate[:-1]], axis=0)
        extended = with_halo(iterate, (("space", 1),), 1)
        extended = jnp.pad(extended, ((0, 0), (0, 0), (1, 1), (1, 1)))
        residual = (
            forcing
            - ((1.0 + 6.0 * coupling) * iterate - coupled(extended, coupling, advect))
            + previous
        )
        scaled = residual * time_weight
        spectrum = forward(lax.all_to_all(scaled, "tm", split_axis=2, concat_axis=0, tiled=True))
        blocked = lax.all_to_all(spectrum, "tm", split_axis=1, concat_axis=3, tiled=True)
        frequency = (time_index * local_steps + jnp.arange(local_steps, dtype=jnp.int32)).astype(
            jnp.float32
        )

        def extend_narrow(field):
            grown = with_halo(field, (("space", 2),), 1)
            return jnp.pad(grown, ((0, 0), (0, 0), (0, 0), (1, 1), (1, 1)))

        solved = jacobi(blocked, coupling, advect, frequency, total_steps, extend_narrow)
        spectrum_out = lax.all_to_all(solved, "tm", split_axis=3, concat_axis=1, tiled=True)
        inverse_part = (
            matmul(cosine, spectrum_out[0].reshape(total_steps, -1))
            - matmul(sine_table, spectrum_out[1].reshape(total_steps, -1))
        ) / total_steps
        inverse_part = inverse_part.reshape(spectrum_out.shape[1:])
        correction = lax.all_to_all(inverse_part, "tm", split_axis=0, concat_axis=2, tiled=True)
        iterate = iterate + correction / time_weight
    return iterate


def body(forcing, initial, coupling, velocity):
    groups = lax.axis_size("tm")
    planes, height, width = initial.shape
    fits = (
        ITERS == 2
        and forcing.shape[0] == 1
        and groups % 4 == 0
        and lax.axis_size("space") == 2
        and 2 * planes == SUB
        and width == LANES
        and height % (groups * SUB) == 0
        and height // (groups // 2) + 1 >= HALO
    )
    plan = banded_body if fits else general_body
    return plan(forcing, initial, coupling, velocity)


def solution(mesh):
    return jax.shard_map(
        body,
        mesh=mesh,
        in_specs=(
            P("tm", "space", None, None),
            P("space", None, None),
            P("space", None, None),
            P(None, "space", None, None),
        ),
        out_specs=P("tm", "space", None, None),
        check_vma=False,
    )
```

```python
import functools
import math

import jax
import jax.numpy as jnp
from jax import lax
from jax.experimental import pallas as pl
from jax.experimental.pallas import tpu as pltpu
from jax.sharding import PartitionSpec as P

ITERS = 2
SWEEPS = 8

wrap_alpha = 0.1

APPS = SWEEPS + 1
HALO = ITERS * APPS - 1
FIRST_GROUPS = 2
SECOND_GROUPS = 2
PREPARED = 4
LANES = 128
SUB = 8


def position(site):
    a, b = site // 2, site % 2
    return 2 * a + (b ^ (a % 2))


def vmem_call(kernel, out_shapes, n_in, scratch=(), n_smem=0, flops=0, limit=8 << 20):
    specs = [pl.BlockSpec(memory_space=pltpu.SMEM)] * n_smem
    specs += [pl.BlockSpec(memory_space=pltpu.VMEM)] * n_in
    multi = isinstance(out_shapes, (tuple, list))
    outs = pl.BlockSpec(memory_space=pltpu.VMEM)
    return pl.pallas_call(
        kernel,
        out_shape=out_shapes,
        in_specs=specs,
        out_specs=[outs] * len(out_shapes) if multi else outs,
        scratch_shapes=list(scratch),
        compiler_params=pltpu.CompilerParams(vmem_limit_bytes=limit),
        cost_estimate=pl.CostEstimate(flops=flops, bytes_accessed=1 << 20, transcendentals=0),
    )


def pack_kernel(sites, rows, f_ref, o_ref):
    planes, total = f_ref.shape[0], f_ref.shape[1]
    block = (rows + 2) * planes
    for site in range(sites):
        first = position(site) * rows
        base = site * block
        for z in range(planes):
            for part in range(rows // SUB):
                tile = f_ref[z, pl.ds(first + part * SUB, SUB), :]
                o_ref[pl.ds(base + (1 + part * SUB) * planes + z, SUB, stride=planes), :] = tile
            for idx, row in ((0, first - 1), (rows + 1, first + rows)):
                if 0 <= row < total:
                    edge = f_ref[z, pl.ds(row, 1), :]
                else:
                    edge = jnp.zeros((1, LANES), jnp.float32)
                o_ref[pl.ds(base + idx * planes + z, 1), :] = edge


def unpack_kernel(sites, rows, ints, r_ref, i_ref, o_ref):
    core = ints[0]
    planes = i_ref.shape[0]
    half = rows // 2
    for site in range(sites):
        first = position(site) * rows
        for part in range(2):
            who = core if part == 0 else 1 - core
            base = (site * 2 + part) * half * planes
            for z in range(planes):
                for piece in range(half // SUB):
                    row = pl.multiple_of(first + who * half + piece * SUB, SUB)
                    tile = r_ref[pl.ds(base + piece * SUB * planes + z, SUB, stride=planes), :]
                    o_ref[0, z, pl.ds(row, SUB), :] = i_ref[z, pl.ds(row, SUB), :] + tile


def shifts(mid, low, high, left, right, coefs):
    depth = mid.shape[0]
    zp, zm, yp, ym, xp, xm = coefs
    out = zp * pltpu.roll(mid, depth - 1, 0) + zm * pltpu.roll(mid, 1, 0)
    out = out + (yp * high + ym * low)
    return out + (xp * left + xm * right)


def moved(mid):
    return pltpu.roll(mid, LANES - 1, 1), pltpu.roll(mid, 1, 1)


def merge_kernel(ints, keep_ref, got_ref, share_ref, o_ref, blob_ref):
    side = ints[1]
    sub = lax.broadcasted_iota(jnp.int32, (SUB, LANES), 0)
    steps, pairs = keep_ref.shape[:2]
    for i in range(steps):
        for pair in range(pairs):
            a, b = keep_ref[i, pair], got_ref[i, pair]
            low = jnp.where(side == 0, a, b)
            high = jnp.where(side == 0, b, a)
            tiles = (
                jnp.where(sub < SUB // 2, low, pltpu.roll(high, SUB // 2, 0)),
                jnp.where(sub < SUB // 2, pltpu.roll(low, SUB // 2, 0), high),
            )
            for h in range(2):
                o_ref[2 * pair + h, i] = tiles[h]
                blob_ref[(2 * pair + h) * steps + i] = tiles[h]
    at = 2 * pairs * steps
    for field in range(share_ref.shape[0]):
        for z in range(share_ref.shape[1]):
            for piece in range(share_ref.shape[2] // SUB):
                blob_ref[at] = share_ref[field, z, pl.ds(piece * SUB, SUB), :]
                at += 1


def prepare_kernel(steps, skip, half, ints, floats, coef_ref, c_ref, p_ref, g_ref):
    wrap = floats[0]
    skip = skip + half * ints[0]
    count = c_ref.shape[0]
    tile = coef_ref.shape[2:]
    z = lax.broadcasted_iota(jnp.int32, tile, 0)
    x = lax.broadcasted_iota(jnp.int32, tile, 1)

    def group_body(i, carry):
        states = [coef_ref[i * PREPARED + skip + u, 4] for u in range(PREPARED)]
        sides = [moved(state) for state in states]
        for u in range(PREPARED):
            row = i * PREPARED + u
            at = row + skip
            coupling = coef_ref[at, 0]
            coefs = []
            for k in range(3):
                advect = coupling * coef_ref[at, 1 + k]
                plus, minus = coupling - advect, coupling + advect
                if k == 0:
                    plus = jnp.where(z == tile[0] - 1, 0.0, plus)
                    minus = jnp.where(z == 0, 0.0, minus)
                if k == 2:
                    plus = jnp.where(x == LANES - 1, 0.0, plus)
                    minus = jnp.where(x == 0, 0.0, minus)
                coefs += [plus, minus]
            inv = 1.0 / (1.0 + 6.0 * coupling)
            for k, value in enumerate(coefs + [inv]):
                c_ref[row, k] = value
            powers = [inv]
            for _ in range(steps - 1):
                powers.append(powers[-1] * inv)
            scale = wrap / (1.0 - wrap * powers[-1])
            for n in range(steps):
                p_ref[row, n] = scale * powers[n]
            around = shifts(states[u], coef_ref[at - 1, 4], coef_ref[at + 1, 4], *sides[u], coefs)
            g_ref[row] = (around - 6.0 * coupling * states[u]) * (1.0 + wrap)
        return carry

    lax.fori_loop(0, count // PREPARED, group_body, 0)


def apply_rows(
    lo, base, count, groups, steps, src, dst, move, side_ref, s_ref, c_ref, p_ref, more, then, fix
):
    size = -(-count // groups)

    def solve(r):
        for u in range(size):
            at = r + u + base
            coefs = [c_ref[at, k] for k in range(6)]
            inv = c_ref[at, 6]
            run = None
            ys = []
            for n in range(steps):
                b = s_ref[at, n]
                if n == 0 and fix is not None:
                    b = b - fix(r + u)
                if more:
                    b = b + shifts(
                        src[r + u, n],
                        src[r + u - 1, n],
                        src[r + u + 1, n],
                        side_ref[u, n, 0],
                        side_ref[u, n, 1],
                        coefs,
                    )
                run = b * inv if run is None else (b + run) * inv
                ys.append(run)
            for n in range(steps):
                dst[r + u - move, n] = ys[n] + ys[-1] * p_ref[at, n]

    def group_body(i, carry):
        r = lo + i * size
        coming = take_sides(src, r + size, size, steps) if more else None
        solve(r)
        if more:
            put_sides(side_ref, coming, steps)
        return carry

    lax.fori_loop(0, groups - 1, group_body, 0)
    early = then is not None and then[0] + then[1] <= lo + (groups - 1) * size
    coming = take_sides(dst, *then, steps) if early else None
    solve(lo + (groups - 1) * size)
    if then is not None:
        put_sides(side_ref, coming if early else take_sides(dst, *then, steps), steps)


def take_sides(ref, r, size, steps):
    return [[moved(ref[r + u, n]) for n in range(steps)] for u in range(size)]


def put_sides(side_ref, values, steps):
    for u, row in enumerate(values):
        for n in range(steps):
            side_ref[u, n, 0], side_ref[u, n, 1] = row[n]


def first_kernel(rows, steps, ints, *refs):
    band_ref, mate_ref, one_ref, mate_one_ref, two_ref, mate_two_ref = refs[:6]
    c_ref, p_ref, g_ref = refs[6:9]
    x_out, s_ref, last_out = refs[9:12]
    x0, x1, side_ref = refs[12:]
    core, odd = ints[0], ints[2]
    half = rows // 2
    skip = half * core
    per = steps // 2

    for idx in range(1, rows + 1):
        j = idx - 1 + HALO - skip
        for i in range(per):
            s_ref[j, 2 * i + core] = band_ref[idx, i] + g_ref[j]
            s_ref[j, 2 * i + 1 - core] = mate_ref[idx * per + i] + g_ref[j]

    def fill(pair, idx, j):
        for i in range(per):
            s_ref[j, 2 * i + core] = pair[0][idx, i] + g_ref[j]
            s_ref[j, 2 * i + 1 - core] = pair[1][idx, i] + g_ref[j]

    for row in range(half + 2 * HALO, s_ref.shape[0]):
        for n in range(steps):
            s_ref[row, n] = jnp.zeros_like(g_ref[0])
    tail = jnp.minimum(s_ref.shape[0] - HALO - rows + skip, rows + 1)
    for pair, previous in (((one_ref, mate_one_ref), odd), ((two_ref, mate_two_ref), 1 - odd)):

        def before(idx, carry):
            fill(pair, idx + rows + 1 - HALO, idx - skip)
            return carry

        def after(idx, carry):
            fill(pair, idx, idx - 1 + HALO + rows - skip)
            return carry

        lax.fori_loop(jnp.where(previous == 1, skip, HALO), HALO, before, 0)
        lax.fori_loop(1, jnp.where(previous == 1, 1, 1 + tail), after, 0)

    bufs = (x0, x1)
    for k in range(1, APPS + 1):
        reach = HALO + 1 - k
        final = k == APPS
        apply_rows(
            HALO - reach,
            0,
            half + 2 * reach,
            FIRST_GROUPS,
            steps,
            bufs[k % 2],
            x_out if final else bufs[(k + 1) % 2],
            HALO - reach if final else 0,
            side_ref,
            s_ref,
            c_ref,
            p_ref,
            k > 1,
            None if final else (HALO - reach + 1, -(-(half + 2 * reach - 2) // FIRST_GROUPS)),
            None,
        )
    for i in range(last_out.shape[0]):
        last_out[i] = x_out[i + 1, steps - 1]


def second_kernel(rows, steps, ints, floats, x_ref, s_ref, last_ref, other_ref, c_ref, p_ref, *refs):
    keep_near, keep_far, send_near, send_far = refs[:4]
    xa, xb, side_ref = refs[4:]
    core, side = ints[0], ints[1]
    wrap = floats[0]
    half = rows // 2
    reach = HALO - APPS
    base = HALO - reach - 1
    count = last_ref.shape[0]

    def fix(r):
        at = jnp.minimum(r - 1, count - 1)
        return (0.5 * wrap) * (last_ref[at] - other_ref[at])

    src, dst = x_ref, xa
    size = -(-(half + 2 * reach) // SECOND_GROUPS)
    put_sides(side_ref, take_sides(x_ref, 1, size, steps), steps)
    for k in range(1, APPS + 1):
        left = reach + 1 - k
        lo = 1 + reach - left
        then = (lo + 1, -(-(half + 2 * left - 2) // SECOND_GROUPS)) if k < APPS else None
        apply_rows(
            lo,
            base,
            half + 2 * left,
            SECOND_GROUPS,
            steps,
            src,
            dst,
            0,
            side_ref,
            s_ref,
            c_ref,
            p_ref,
            True,
            then,
            fix,
        )
        src, dst = dst, (xb if dst is xa else xa)
    sub = lax.broadcasted_iota(jnp.int32, (SUB, LANES), 0)
    for pair in range(half // 2):
        for i in range(steps // 2):
            for to_core, near, far in ((0, keep_near, keep_far), (1, send_near, send_far)):
                parity = core if to_core == 0 else 1 - core
                a = src[1 + reach + 2 * pair, 2 * i + parity]
                b = src[1 + reach + 2 * pair + 1, 2 * i + parity]
                low = jnp.where(sub < SUB // 2, a, pltpu.roll(b, SUB // 2, 0))
                high = jnp.where(sub < SUB // 2, pltpu.roll(a, SUB // 2, 0), b)
                near[i, pair] = jnp.where(side == 0, low, high)
                far[i, pair] = jnp.where(side == 0, high, low)


def banded_body(forcing, initial, coupling, velocity):
    f32 = jnp.float32
    groups = lax.axis_size("tm")
    sites = groups // 2
    steps = groups // 2
    planes, height, width = initial.shape
    rows = height // sites
    half = rows // 2
    depth = 2 * planes
    tile = (depth, width)
    time_index = lax.axis_index("tm")
    side = lax.axis_index("space")
    core = time_index % 2
    site = time_index // 2
    place = position(site)
    root = math.sqrt(wrap_alpha)
    wrap = jnp.where(side == 0, root, -root).astype(f32)
    window = -(-(half + 2 * HALO) // PREPARED) * PREPARED
    margin = (-(-(rows + 2 * (HALO + 1)) // SUB) * SUB - rows) // 2
    ints = jnp.stack([core, side, place % 2]).astype(jnp.int32)
    floats = wrap[None]

    same_core = [[2 * i + c for i in range(sites)] for c in range(2)]
    cores = [(i, i ^ 1) for i in range(groups)]
    sides = [(0, 1), (1, 0)]
    by_place = {position(q): q for q in range(sites)}

    def exchange(first):
        both = []
        for p in range(first, sites - 1, 2):
            for c in range(2):
                one, two = 2 * by_place[p] + c, 2 * by_place[p + 1] + c
                both += [(one, two), (two, one)]
        return both

    fields = jnp.concatenate([coupling[None], velocity, initial[None]], axis=0)
    padded = jnp.pad(fields, ((0, 0), (0, 0), (margin, margin), (0, 0)))
    mine = lax.dynamic_slice_in_dim(padded, place * rows, rows + 2 * margin, axis=2)
    share = lax.dynamic_slice_in_dim(mine, core * (planes // 2), planes // 2, axis=1)
    share = lax.ppermute(share, "space", sides)

    packed = vmem_call(
        functools.partial(pack_kernel, sites, rows),
        jax.ShapeDtypeStruct((sites * (rows + 2) * planes, width), f32),
        1,
    )(forcing[0])
    packed = packed.reshape(sites, (rows + 2) // 2, 2 * planes, width)
    arrived = lax.all_to_all(
        packed, "tm", split_axis=0, concat_axis=0, tiled=True, axis_index_groups=same_core
    )
    near, far = arrived[: steps // 2], arrived[steps // 2 :]
    keep = near + wrap * far
    send = near - wrap * far
    got = lax.ppermute(send, "space", sides)
    tiles = (rows + 2) * (steps // 2)
    band, blob = vmem_call(
        merge_kernel,
        [
            jax.ShapeDtypeStruct((rows + 2, steps // 2) + tile, f32),
            jax.ShapeDtypeStruct((tiles + share.size // (SUB * width), SUB, width), f32),
        ],
        3,
        n_smem=1,
    )(ints, keep, got, share)
    one = lax.ppermute(band, "tm", exchange(0))
    two = lax.ppermute(band, "tm", exchange(1))
    mate = lax.ppermute(blob, "tm", cores)
    mate_share = mate[tiles:].reshape(share.shape)

    low, high = jnp.where(core == 0, share, mate_share), jnp.where(core == 0, mate_share, share)
    theirs = jnp.concatenate([low, high], axis=1)
    halves = jnp.where(side == 0, mine, theirs), jnp.where(side == 0, theirs, mine)
    coefs = jnp.concatenate(halves, axis=1).transpose(2, 0, 1, 3)
    weights, wraps, extra = vmem_call(
        functools.partial(prepare_kernel, steps, margin - HALO, half),
        [
            jax.ShapeDtypeStruct((window, 7) + tile, f32),
            jax.ShapeDtypeStruct((window, steps) + tile, f32),
            jax.ShapeDtypeStruct((window,) + tile, f32),
        ],
        1,
        n_smem=2,
        flops=5_000_000,
    )(ints, floats, coefs)

    one, two, weights, wraps, extra = lax.optimization_barrier((one, two, weights, wraps, extra))
    mate_one = lax.ppermute(one, "tm", cores)
    mate_two = lax.ppermute(two, "tm", cores)

    reach = HALO + 1 - APPS
    limit = 12 * 1024 * 1024
    spare = SUB
    x_mid, source, last = vmem_call(
        functools.partial(first_kernel, rows, steps),
        [
            jax.ShapeDtypeStruct((half + 2 * reach + spare, steps) + tile, f32),
            jax.ShapeDtypeStruct((window, steps) + tile, f32),
            jax.ShapeDtypeStruct((half + 2 * reach - 2,) + tile, f32),
        ],
        9,
        scratch=[
            pltpu.VMEM((window + spare, steps) + tile, f32),
            pltpu.VMEM((window + spare, steps) + tile, f32),
            pltpu.VMEM((-(-(half + 2 * HALO) // FIRST_GROUPS), steps, 2) + tile, f32),
        ],
        n_smem=1,
        flops=20_000_000,
        limit=limit,
    )(ints, band, mate, one, mate_one, two, mate_two, weights, wraps, extra)
    other = lax.ppermute(last, "space", sides)
    quarter = jax.ShapeDtypeStruct((steps // 2, half // 2) + tile, f32)
    keep_near, keep_far, send_near, send_far = vmem_call(
        functools.partial(second_kernel, rows, steps),
        [quarter] * 4,
        6,
        scratch=[
            pltpu.VMEM((half + 2 * reach + spare, steps) + tile, f32),
            pltpu.VMEM((half + 2 * reach + spare, steps) + tile, f32),
            pltpu.VMEM((-(-(half + 2 * reach) // SECOND_GROUPS), steps, 2) + tile, f32),
        ],
        n_smem=2,
        flops=10_000_000,
        limit=limit,
    )(ints, floats, x_mid, source, last, other, weights, wraps)

    got_near = lax.ppermute(send_near, "tm", cores)
    got_far = lax.ppermute(send_far, "tm", cores)
    mate_near = lax.ppermute(keep_far, "space", sides)
    mate_far = lax.ppermute(got_far, "space", sides)
    ours = jnp.stack([keep_near, got_near], axis=1)
    mates = jnp.stack([mate_near, mate_far], axis=1)
    early = 0.5 * (ours + mates)
    late = (0.5 / wrap) * (ours - mates)
    result = jnp.concatenate([early, late], axis=0)
    spread = lax.all_to_all(
        result, "tm", split_axis=0, concat_axis=0, tiled=True, axis_index_groups=same_core
    )
    return vmem_call(
        functools.partial(unpack_kernel, sites, rows),
        jax.ShapeDtypeStruct((1, planes, height, width), f32),
        2,
        n_smem=1,
    )(ints, spread.reshape(-1, width), initial)


def passed_along(array, axis, by):
    size = lax.axis_size(axis)
    pairs = [(i, i + by) for i in range(size) if 0 <= i + by < size]
    return lax.ppermute(array, axis, pairs)


def with_halo(block, sides, width):
    for axis, dim in sides:
        count = lax.axis_size(axis)
        forward = [(i, i + 1) for i in range(count - 1)]
        backward = [(target, source) for source, target in forward]
        low = lax.ppermute(
            lax.slice_in_dim(block, block.shape[dim] - width, None, axis=dim), axis, forward
        )
        high = lax.ppermute(lax.slice_in_dim(block, 0, width, axis=dim), axis, backward)
        block = jnp.concatenate([low, block, high], axis=dim)
    return block


def coupled(extended, coupling, advect):
    total = (coupling - advect[0]) * extended[..., 2:, 1:-1, 1:-1] + (
        coupling + advect[0]
    ) * extended[..., :-2, 1:-1, 1:-1]
    total = (
        total
        + (coupling - advect[1]) * extended[..., 1:-1, 2:, 1:-1]
        + (coupling + advect[1]) * extended[..., 1:-1, :-2, 1:-1]
    )
    total = (
        total
        + (coupling - advect[2]) * extended[..., 1:-1, 1:-1, 2:]
        + (coupling + advect[2]) * extended[..., 1:-1, 1:-1, :-2]
    )
    return total


def tables(total_steps):
    indices = jnp.arange(total_steps, dtype=jnp.int32)
    products = indices[:, None] * indices[None, :] % total_steps
    angles = products.astype(jnp.float32) * (2.0 * math.pi / total_steps)
    return (jnp.cos(angles), jnp.sin(angles))


def matmul(table, columns):
    return jnp.dot(
        table, columns, preferred_element_type=jnp.float32, precision=lax.Precision.HIGHEST
    )


def jacobi(spectrum, coupling, advect, frequency, total_steps, extend):
    radius = math.exp(math.log(wrap_alpha) / total_steps)
    angles = (frequency * (2.0 * math.pi / total_steps))[:, None, None, None]
    diag_re = 1.0 + 6.0 * coupling - radius * jnp.cos(angles)
    diag_im = radius * jnp.sin(angles) + jnp.zeros_like(diag_re)
    modulus = diag_re * diag_re + diag_im * diag_im
    source_re = spectrum[0]
    source_im = spectrum[1]
    value_re = (source_re * diag_re + source_im * diag_im) / modulus
    value_im = (source_im * diag_re - source_re * diag_im) / modulus
    for _ in range(SWEEPS):
        extended = extend(jnp.stack([value_re, value_im]))
        summed = coupled(extended, coupling, advect)
        sum_re = source_re + summed[0]
        sum_im = source_im + summed[1]
        value_re = (sum_re * diag_re + sum_im * diag_im) / modulus
        value_im = (sum_im * diag_re - sum_re * diag_im) / modulus
    return jnp.stack([value_re, value_im])


def general_body(forcing, initial, coupling, velocity):
    local_steps = forcing.shape[0]
    groups = lax.axis_size("tm")
    total_steps = local_steps * groups
    time_index = lax.axis_index("tm")
    advect = coupling[None] * velocity
    cosine, sine_table = tables(total_steps)
    global_steps = (time_index * local_steps + jnp.arange(local_steps, dtype=jnp.int32)).astype(
        jnp.float32
    )
    time_weight = jnp.exp(math.log(wrap_alpha) * global_steps / total_steps)[:, None, None, None]
    iterate = jnp.broadcast_to(initial, forcing.shape)

    def forward(piece):
        columns = piece.reshape(piece.shape[0], -1)
        spec_re = matmul(cosine, columns)
        spec_im = -matmul(sine_table, columns)
        return jnp.stack([spec_re, spec_im]).reshape((2,) + piece.shape)

    for _ in range(ITERS):
        before = passed_along(iterate[-1], "tm", 1)
        before = jnp.where(time_index == 0, initial, before)
        previous = jnp.concatenate([before[None], iterate[:-1]], axis=0)
        extended = with_halo(iterate, (("space", 1),), 1)
        extended = jnp.pad(extended, ((0, 0), (0, 0), (1, 1), (1, 1)))
        residual = (
            forcing
            - ((1.0 + 6.0 * coupling) * iterate - coupled(extended, coupling, advect))
            + previous
        )
        scaled = residual * time_weight
        spectrum = forward(lax.all_to_all(scaled, "tm", split_axis=2, concat_axis=0, tiled=True))
        blocked = lax.all_to_all(spectrum, "tm", split_axis=1, concat_axis=3, tiled=True)
        frequency = (time_index * local_steps + jnp.arange(local_steps, dtype=jnp.int32)).astype(
            jnp.float32
        )

        def extend_narrow(field):
            grown = with_halo(field, (("space", 2),), 1)
            return jnp.pad(grown, ((0, 0), (0, 0), (0, 0), (1, 1), (1, 1)))

        solved = jacobi(blocked, coupling, advect, frequency, total_steps, extend_narrow)
        spectrum_out = lax.all_to_all(solved, "tm", split_axis=3, concat_axis=1, tiled=True)
        inverse_part = (
            matmul(cosine, spectrum_out[0].reshape(total_steps, -1))
            - matmul(sine_table, spectrum_out[1].reshape(total_steps, -1))
        ) / total_steps
        inverse_part = inverse_part.reshape(spectrum_out.shape[1:])
        correction = lax.all_to_all(inverse_part, "tm", split_axis=0, concat_axis=2, tiled=True)
        iterate = iterate + correction / time_weight
    return iterate


def body(forcing, initial, coupling, velocity):
    groups = lax.axis_size("tm")
    planes, height, width = initial.shape
    fits = (
        ITERS == 2
        and forcing.shape[0] == 1
        and groups % 4 == 0
        and lax.axis_size("space") == 2
        and 2 * planes == SUB
        and width == LANES
        and height % (groups * SUB) == 0
        and height // (groups // 2) + 1 >= HALO
    )
    plan = banded_body if fits else general_body
    return plan(forcing, initial, coupling, velocity)


def solution(mesh):
    return jax.shard_map(
        body,
        mesh=mesh,
        in_specs=(
            P("tm", "space", None, None),
            P("space", None, None),
            P("space", None, None),
            P(None, "space", None, None),
        ),
        out_specs=P("tm", "space", None, None),
        check_vma=False,
    )
```
